32 devices in a mesh: lat: 4 (over z), lon: 4 (over y, x), lev: 2 (over core).
Axes of the slice: x: 2, y: 2, z: 4, core: 2. Of those that a mesh axis runs over, the one named last changes fastest.
Arguments:
- pressure: float32 [16, 256, 128, 128], P('lat', 'lon', 'lev'), may hold values from 0.2 to 1.8
- earlier: float32 [16, 256, 128, 128], P('lat', 'lon', 'lev'), may hold values from 0.2 to 1.8
- speed_square: float32 [16, 256, 128, 128], P('lat', 'lon', 'lev'), may hold values from 0.05 to 0.3
Outputs:
- pressure_end: float32 [16, 256, 128, 128], P('lat', 'lon', 'lev')
The draws below stay inside these ranges and needn't reach their ends.
All inputs are finite; a program needn't handle non-finite values.
Results may differ from the reference program's by a relative error of at most 0.00002.
Values sent between devices are 32-bit elements.
No kernel may reach another device: no remote copies, remote signals or barrier semaphores. Data moves between devices by JAX's collectives and lax.ppermute only.
A program may use at most 320 MiB of HBM per device.

```python
import jax
import jax.numpy as jnp
from jax import lax

GRID_Y = 16
GRID_X = 256
GRID_Z = 128
LEVELS = 128
STEPS = 4


def block_levels(stream_key, extent, cuts, least, high):
    def one(dim, shards_of):
        steps = jax.random.uniform(jax.random.fold_in(jax.random.fold_in(stream_key, 6), dim), (shards_of,), jnp.float32, least / len(cuts), high / len(cuts))
        return jnp.repeat(jnp.exp(steps), extent[dim] // shards_of).reshape((-1,) + (1,) * (len(extent) - dim - 1))

    factor_of = one(*cuts[0])
    for cut in cuts[1:]:
        factor_of = factor_of * one(*cut)
    return factor_of


def setup_inputs(seed: int = 0) -> dict:
    splits = jax.random.split(jax.random.key(seed), 4)
    return {
        "pressure": jnp.clip(0.2 + 1.5999999 * jax.random.uniform(splits[0], (GRID_Y, GRID_X, GRID_Z, LEVELS), jnp.float32) ** block_levels(splits[0], (GRID_Y, GRID_X, GRID_Z, LEVELS), ((0, 4), (1, 4), (2, 2)), -0.2, 0.2), 0.2, 1.8),
        "earlier": jnp.clip(0.2 + 1.5999999 * jax.random.uniform(splits[1], (GRID_Y, GRID_X, GRID_Z, LEVELS), jnp.float32) ** block_levels(splits[1], (GRID_Y, GRID_X, GRID_Z, LEVELS), ((0, 4), (1, 4), (2, 2)), -0.2, 0.2), 0.2, 1.8),
        "speed_square": jnp.clip(0.05 + 0.25 * jax.random.uniform(splits[2], (GRID_Y, GRID_X, GRID_Z, LEVELS), jnp.float32) ** block_levels(splits[2], (GRID_Y, GRID_X, GRID_Z, LEVELS), ((0, 4), (1, 4), (2, 2)), -0.2, 0.2), 0.05, 0.3),
    }


def inner_cells(values, dims):
    for dim in dims:
        values = lax.slice_in_dim(values, 1, values.shape[dim] - 1, axis=dim)
    return values


def side_cells(values, dim, start, dims):
    others = [other for other in dims if other != dim]
    values = inner_cells(values, others)
    return lax.slice_in_dim(values, start, start + values.shape[dim] - 2, axis=dim)


def advance(padded, before, speed_square):
    middle = inner_cells(padded, (0, 1, 2))
    lower = [side_cells(padded, dim, 0, (0, 1, 2)) for dim in (0, 1, 2)]
    upper = [side_cells(padded, dim, 2, (0, 1, 2)) for dim in (0, 1, 2)]
    spread = lower[0] + upper[0] + lower[1] + upper[1] + lower[2] + upper[2] - 6.0 * middle
    return 2.0 * middle - before + speed_square * spread


def reference(pressure, earlier, speed_square):
    for step in range(STEPS):
        later = advance(jnp.pad(pressure, ((1, 1), (1, 1), (1, 1), (0, 0)), mode="constant"), earlier, speed_square)
        earlier, pressure = pressure, later
    return pressure
```

```python
import functools

import jax
import jax.numpy as jnp
from jax import lax
from jax.experimental import pallas as pl
from jax.experimental.pallas import tpu as pltpu
from jax.sharding import PartitionSpec as P

STEPS = 4
CHUNKS = 2


def divisor(extent, most):
    return next(size for size in range(min(extent, most), 0, -1) if extent % size == 0)


def shifted(axis, upward, values):
    count = lax.axis_size(axis)
    pairs = [(i, i + 1) for i in range(count - 1)]
    if not upward:
        pairs = [(target, source) for source, target in pairs]
    return lax.ppermute(values, axis, pairs)


def inner_kernel(field, before, after, earlier, speed, x_low, x_high, z_low, z_high, out):
    rows, width, depth, _ = field.shape
    block, last = pl.program_id(0), pl.num_programs(0) - 1
    row = lax.broadcasted_iota(jnp.int32, field.shape[2:], 0)

    def cell(y, x, left, right):
        middle = field[y, x]
        down = jnp.where(row == 0, z_low[y, pl.ds(x, 1)], pltpu.roll(middle, 1, 0))
        up = jnp.where(row == depth - 1, z_high[y, pl.ds(x, 1)], pltpu.roll(middle, depth - 1, 0))
        total = left + right + down + up
        if y > 0:
            total = total + field[y - 1, x]
        if y < rows - 1:
            total = total + field[y + 1, x]
        out[y, x] = 2.0 * middle - earlier[y, x] + speed[y, x] * (total - 6.0 * middle)

    for y in range(rows):
        left = jnp.where(block == 0, x_low[y], before[y, 0])
        cell(y, 0, left, field[y, 1])
        right = jnp.where(block == last, x_high[y], after[y, 0])
        cell(y, width - 1, field[y, width - 2], right)

    @pl.loop(1, width - 1)
    def _(x):
        for y in range(rows):
            cell(y, x, field[y, x - 1], field[y, x + 1])


def inner_update(field, earlier, speed, x_low, x_high, z_low, z_high):
    rows, width, depth, levels = field.shape
    step = divisor(width, 8)
    blocks = width // step
    main = pl.BlockSpec((rows, step, depth, levels), lambda b: (0, b, 0, 0))
    slab = (rows, 1, depth, levels)
    whole = pl.BlockSpec((rows, depth, levels), lambda b: (0, 0, 0))
    face = pl.BlockSpec((rows, step, levels), lambda b: (0, b, 0))
    cells = field.size
    return pl.pallas_call(
        inner_kernel,
        grid=(blocks,),
        in_specs=[
            main,
            pl.BlockSpec(slab, lambda b: (0, jnp.maximum(b * step - 1, 0), 0, 0)),
            pl.BlockSpec(slab, lambda b: (0, jnp.minimum((b + 1) * step, width - 1), 0, 0)),
            main,
            main,
            whole,
            whole,
            face,
            face,
        ],
        out_specs=main,
        out_shape=jax.ShapeDtypeStruct(field.shape, field.dtype),
        cost_estimate=pl.CostEstimate(flops=60 * cells, bytes_accessed=16 * cells, transcendentals=0),
        name="inner",
    )(field, field, field, earlier, speed, x_low, x_high, z_low, z_high)


def outer_kernel(partial, speed, low, high, out, *sends):
    side = pl.program_id(0)

    @pl.when(side == 0)
    def _():
        value = partial[0] + speed[0] * low[...]
        out[0] = value
        if sends:
            sends[0][...] = value

    @pl.when(side == 1)
    def _():
        value = partial[0] + speed[0] * high[...]
        out[0] = value
        if sends:
            sends[1][...] = value


def outer_update(partial, speed, low, high, chunk, emit):
    rows, _, depth, levels = partial.shape
    width = low.shape[0]
    step = divisor(width, 8)
    blocks = width // step
    offset = chunk * blocks
    plane = pl.BlockSpec((1, step, depth, levels), lambda s, b: (s * (rows - 1), offset + b, 0, 0))
    first = pl.BlockSpec((step, depth, levels), lambda s, b: (jnp.where(s == 0, b, blocks - 1), 0, 0))
    second = pl.BlockSpec((step, depth, levels), lambda s, b: (jnp.where(s == 0, 0, b), 0, 0))
    piece = jax.ShapeDtypeStruct(low.shape, low.dtype)
    whole = jax.ShapeDtypeStruct(partial.shape, partial.dtype)
    return pl.pallas_call(
        outer_kernel,
        grid=(2, blocks),
        in_specs=[plane, plane, first, second],
        out_specs=[plane] + ([first, second] if emit else []),
        out_shape=[whole] + ([piece, piece] if emit else []),
        input_output_aliases={0: 0},
        cost_estimate=pl.CostEstimate(flops=60 * low.size, bytes_accessed=40 * low.size, transcendentals=0),
        name="outer",
    )(partial, speed, low, high)


def shards(pressure, earlier, speed):
    rows, width, depth, _ = pressure.shape
    chunks = CHUNKS if width % CHUNKS == 0 else 1
    piece = width // chunks

    def exchange(low, high):
        return shifted("lat", True, high), shifted("lat", False, low)

    arrived = []
    for chunk in range(chunks):
        low = lax.slice(pressure, (0, chunk * piece, 0, 0), (1, (chunk + 1) * piece) + pressure.shape[2:])
        high = lax.slice(pressure, (rows - 1, chunk * piece, 0, 0), (rows, (chunk + 1) * piece) + pressure.shape[2:])
        arrived.append(exchange(low[0], high[0]))

    for step in range(STEPS):
        x_low = shifted("lon", True, pressure[:, width - 1])
        x_high = shifted("lon", False, pressure[:, 0])
        z_low = shifted("lev", True, pressure[:, :, depth - 1])
        z_high = shifted("lev", False, pressure[:, :, 0])
        later = inner_update(pressure, earlier, speed, x_low, x_high, z_low, z_high)
        emit = step < STEPS - 1
        coming = []
        for chunk in range(chunks):
            later, *sends = outer_update(later, speed, *arrived[chunk], chunk, emit)
            if emit:
                coming.append(exchange(*sends))
        arrived = coming
        earlier, pressure = pressure, later
    return pressure


def solution(mesh):
    spec = P("lat", "lon", "lev", None)
    return jax.shard_map(shards, mesh=mesh, in_specs=(spec, spec, spec), out_specs=spec, check_vma=False)
```

```python
import functools

import jax
import jax.numpy as jnp
from jax import lax
from jax.experimental import pallas as pl
from jax.experimental.pallas import tpu as pltpu
from jax.sharding import PartitionSpec as P

STEPS = 4
CHUNKS = 2


WHOLE = pl.BlockSpec(memory_space=pltpu.VMEM)
LIMIT = 4 * 1024 * 1024


def call(kernel, args, outs, name, **options):
    cells = sum(arg.size for arg in args) + sum(out.size for out in outs)
    return pl.pallas_call(
        kernel,
        in_specs=[WHOLE] * len(args),
        out_specs=[WHOLE] * len(outs),
        out_shape=[pltpu.VMEM(out.shape, out.dtype) for out in outs],
        cost_estimate=pl.CostEstimate(flops=40 * cells, bytes_accessed=4 * cells, transcendentals=0),
        compiler_params=pltpu.CompilerParams(vmem_limit_bytes=LIMIT),
        name=name,
        **options,
    )(*[pltpu.with_memory_space_constraint(arg, pltpu.VMEM) for arg in args])


def shifted(axis, upward, values):
    count = lax.axis_size(axis)
    pairs = [(i, i + 1) for i in range(count - 1)]
    if not upward:
        pairs = [(target, source) for source, target in pairs]
    return lax.ppermute(values, axis, pairs)


def between(axis, low, high):
    return shifted(axis, True, high), shifted(axis, False, low)


def inner_kernel(swap, field, earlier, speed, x_low, x_high, z_low, z_high, out):
    rows, width, depth, _ = field.shape
    row = lax.broadcasted_iota(jnp.int32, field.shape[2:], 0)
    place = lax.axis_index("lev")
    first, last = place == 0, place == swap - 1

    def column(x, left, right):
        for y in range(rows):
            middle = field[y, x]
            low = jnp.where(first, 0.0, z_low[y, pl.ds(x, 1)])
            high = jnp.where(last, 0.0, z_high[y, pl.ds(x, 1)])
            down = jnp.where(row == 0, low, pltpu.roll(middle, 1, 0))
            up = jnp.where(row == depth - 1, high, pltpu.roll(middle, depth - 1, 0))
            total = left(y) + right(y) + down + up
            if y > 0:
                total = total + field[y - 1, x]
            if y < rows - 1:
                total = total + field[y + 1, x]
            out[y, x] = 2.0 * middle - earlier[y, x] + speed[y, x] * (total - 6.0 * middle)

    column(0, lambda y: x_low[y], lambda y: field[y, 1])
    column(width - 1, lambda y: field[y, width - 2], lambda y: x_high[y])

    @pl.loop(1, width - 1)
    def _(x):
        column(x, lambda y: field[y, x - 1], lambda y: field[y, x + 1])


def emit_faces(swap, field, x_first, x_last, *z_faces):
    rows, width, depth, _ = field.shape
    for y in range(rows):
        x_first[y] = field[y, 0]
        x_last[y] = field[y, width - 1]
        low, high = field[y, :, 0, :], field[y, :, depth - 1, :]
        if len(z_faces) == 1:
            z_faces[0][y] = jnp.where(lax.axis_index("lev") == 0, high, low)
        else:
            z_faces[0][y] = low
            z_faces[1][y] = high


def face_shapes(field, swap):
    rows, width, depth, levels = field.shape
    x_face = jax.ShapeDtypeStruct((rows, depth, levels), field.dtype)
    z_face = jax.ShapeDtypeStruct((rows, width, levels), field.dtype)
    return [x_face] * 2 + [z_face] * (1 if swap == 2 else 2)


def outer_kernel(swap, chunk, partial, speed, low, high, out, send_low, send_high, *faces):
    rows, width = out.shape[0], low.shape[0]

    @pl.loop(0, width)
    def _(x):
        place = chunk * width + x
        value = partial[0, place] + speed[0, place] * low[x]
        out[0, place] = value
        send_low[x] = value
        value = partial[rows - 1, place] + speed[rows - 1, place] * high[x]
        out[rows - 1, place] = value
        send_high[x] = value

    if faces:
        emit_faces(swap, out, *faces)


def last_kernel(chunk, partial, speed, low, high, out):
    rows, width = partial.shape[0], low.shape[0]

    @pl.loop(0, width)
    def _(x):
        place = chunk * width + x
        out[0, place] = partial[0, place] + speed[0, place] * low[x]
        out[rows - 1, place] = partial[rows - 1, place] + speed[rows - 1, place] * high[x]


def shards(pressure, earlier, speed):
    rows, width, depth, levels = pressure.shape
    swap = lax.axis_size("lev")
    chunks = CHUNKS if width % CHUNKS == 0 else 1
    piece = width // chunks
    shape = jax.ShapeDtypeStruct(pressure.shape, pressure.dtype)
    part = jax.ShapeDtypeStruct((piece, depth, levels), pressure.dtype)

    arrived = []
    source = pressure
    for chunk in range(chunks):
        sizes = (1, (chunk + 1) * piece, depth, levels)
        low = lax.slice(source, (0, chunk * piece, 0, 0), sizes)[0]
        high = lax.slice(source, (rows - 1, chunk * piece, 0, 0), (rows,) + sizes[1:])[0]
        low, high, source = lax.optimization_barrier((low, high, source))
        arrived.append(between("lat", low, high))

    faces = call(functools.partial(emit_faces, swap), [pressure], face_shapes(pressure, swap), "faces")
    for step in range(STEPS):
        x_low, x_high = between("lon", faces[0], faces[1])
        if swap == 2:
            z_low = z_high = lax.ppermute(faces[2], "lev", [(0, 1), (1, 0)])
        else:
            z_low, z_high = between("lev", faces[2], faces[3])
        (later,) = call(
            functools.partial(inner_kernel, swap),
            [pressure, earlier, speed, x_low, x_high, z_low, z_high],
            [shape],
            "inner",
        )
        coming = []
        for chunk in range(chunks):
            args = [later, speed, *arrived[chunk]]
            if step == STEPS - 1:
                (later,) = call(
                    functools.partial(last_kernel, chunk), args, [shape], "last", input_output_aliases={0: 0}
                )
                continue
            outs = [shape, part, part] + (face_shapes(pressure, swap) if chunk == chunks - 1 else [])
            later, *sends = call(
                functools.partial(outer_kernel, swap, chunk), args, outs, "outer", input_output_aliases={0: 0}
            )
            coming.append(between("lat", sends[0], sends[1]))
            faces = sends[2:]
        arrived = coming
        earlier, pressure = pressure, later
    return pressure


def solution(mesh):
    spec = P("lat", "lon", "lev", None)
    return jax.shard_map(shards, mesh=mesh, in_specs=(spec, spec, spec), out_specs=spec, check_vma=False)
```

```python
import functools

import jax
import jax.numpy as jnp
from jax import lax
from jax.experimental import pallas as pl
from jax.experimental.pallas import tpu as pltpu
from jax.sharding import PartitionSpec as P

STEPS = 4
CHUNKS = 2


WHOLE = pl.BlockSpec(memory_space=pltpu.VMEM)
LIMIT = 4 * 1024 * 1024


def call(kernel, args, outs, name, **options):
    cells = sum(arg.size for arg in args) + sum(out.size for out in outs)
    return pl.pallas_call(
        kernel,
        in_specs=[WHOLE] * len(args),
        out_specs=[WHOLE] * len(outs),
        out_shape=[pltpu.VMEM(out.shape, out.dtype) for out in outs],
        cost_estimate=pl.CostEstimate(flops=40 * cells, bytes_accessed=4 * cells, transcendentals=0),
        compiler_params=pltpu.CompilerParams(vmem_limit_bytes=LIMIT),
        name=name,
        **options,
    )(*[pltpu.with_memory_space_constraint(arg, pltpu.VMEM) for arg in args])


def rounds(axis):
    return 2 if lax.axis_size(axis) > 2 else 1


def swap(axis, turn, values):
    pairs = [(i, i + 1) for i in range(turn, lax.axis_size(axis) - 1, 2)]
    return lax.ppermute(values, axis, pairs + [(high, low) for low, high in pairs])


def upward(axis, turn):
    return lax.rem(lax.axis_index(axis), 2) == turn


def edge(axis, turn, extent):
    return jnp.where(upward(axis, turn), extent - 1, 0)


def sides(axis, faces):
    if len(faces) == 1:
        return jnp.where(upward(axis, 0), 0.0, faces[0]), jnp.where(upward(axis, 0), faces[0], 0.0)
    return jnp.where(upward(axis, 0), faces[1], faces[0]), jnp.where(upward(axis, 0), faces[0], faces[1])


def inner_kernel(counts, field, earlier, speed, *refs):
    rows, width, depth, _ = field.shape
    x_faces, z_faces, out = refs[: counts[0]], refs[counts[0] : -1], refs[-1]
    row = lax.broadcasted_iota(jnp.int32, field.shape[2:], 0)

    def column(x, left, right):
        for y in range(rows):
            middle = field[y, x]
            low, high = sides("lev", [face[y, pl.ds(x, 1)] for face in z_faces])
            down = jnp.where(row == 0, low, pltpu.roll(middle, 1, 0))
            up = jnp.where(row == depth - 1, high, pltpu.roll(middle, depth - 1, 0))
            total = left(y) + right(y) + down + up
            if y > 0:
                total = total + field[y - 1, x]
            if y < rows - 1:
                total = total + field[y + 1, x]
            out[y, x] = 2.0 * middle - earlier[y, x] + speed[y, x] * (total - 6.0 * middle)

    def x_side(y, side):
        return sides("lon", [face[y] for face in x_faces])[side]

    column(0, lambda y: x_side(y, 0), lambda y: field[y, 1])
    column(width - 1, lambda y: field[y, width - 2], lambda y: x_side(y, 1))

    @pl.loop(1, width - 1)
    def _(x):
        column(x, lambda y: field[y, x - 1], lambda y: field[y, x + 1])


def emit_faces(counts, field, *faces):
    rows, width, depth, _ = field.shape
    for y in range(rows):
        for turn, face in enumerate(faces[: counts[0]]):
            face[y] = field[y, edge("lon", turn, width)]
        low, high = field[y, :, 0, :], field[y, :, depth - 1, :]
        for turn, face in enumerate(faces[counts[0] :]):
            face[y] = jnp.where(upward("lev", turn), high, low)


def face_shapes(field, counts):
    rows, width, depth, levels = field.shape
    x_face = jax.ShapeDtypeStruct((rows, depth, levels), field.dtype)
    z_face = jax.ShapeDtypeStruct((rows, width, levels), field.dtype)
    return [x_face] * counts[0] + [z_face] * counts[1]


def outer_kernel(counts, chunk, turns, emit, partial, speed, *refs):
    halos, out, sends, faces = refs[:turns], refs[turns], refs[turns + 1 :], refs[2 * turns + 1 :]
    rows, width = out.shape[0], halos[0].shape[0]

    @pl.loop(0, width)
    def _(x):
        place = chunk * width + x
        for turn, halo in enumerate(halos):
            y = edge("lat", turn, rows)
            value = partial[y, place] + speed[y, place] * halo[x]
            out[y, place] = value
            if emit:
                sends[turn][x] = value

    if faces:
        emit_faces(counts, out, *faces)


def shards(pressure, earlier, speed):
    rows, width, depth, levels = pressure.shape
    chunks = CHUNKS if width % CHUNKS == 0 else 1
    piece = width // chunks
    turns, counts = rounds("lat"), (rounds("lon"), rounds("lev"))
    shape = jax.ShapeDtypeStruct(pressure.shape, pressure.dtype)
    part = jax.ShapeDtypeStruct((piece, depth, levels), pressure.dtype)

    arrived = []
    source = pressure
    for chunk in range(chunks):
        sends = []
        for turn in range(turns):
            start = (edge("lat", turn, rows), chunk * piece, 0, 0)
            sends.append(lax.dynamic_slice(source, start, (1,) + part.shape)[0])
        *sends, source = lax.optimization_barrier((*sends, source))
        arrived.append([swap("lat", turn, send) for turn, send in enumerate(sends)])

    faces = call(functools.partial(emit_faces, counts), [pressure], face_shapes(pressure, counts), "faces")
    for step in range(STEPS):
        x_faces = [swap("lon", turn, face) for turn, face in enumerate(faces[: counts[0]])]
        z_faces = [swap("lev", turn, face) for turn, face in enumerate(faces[counts[0] :])]
        (later,) = call(
            functools.partial(inner_kernel, counts),
            [pressure, earlier, speed, *x_faces, *z_faces],
            [shape],
            "inner",
        )
        emit = step < STEPS - 1
        coming = []
        for chunk in range(chunks):
            outs = [shape]
            if emit:
                outs += [part] * turns
                if chunk == chunks - 1:
                    outs += face_shapes(pressure, counts)
            later, *sends = call(
                functools.partial(outer_kernel, counts, chunk, turns, emit),
                [later, speed, *arrived[chunk]],
                outs,
                "outer",
                input_output_aliases={0: 0},
            )
            if emit:
                coming.append([swap("lat", turn, send) for turn, send in enumerate(sends[:turns])])
                faces = sends[turns:]
        arrived = coming
        earlier, pressure = pressure, later
    return pressure


def solution(mesh):
    spec = P("lat", "lon", "lev", None)
    return jax.shard_map(shards, mesh=mesh, in_specs=(spec, spec, spec), out_specs=spec, check_vma=False)
```
